32 devices in a mesh: dp: 4 (over x, core), tensor: 8 (over z, y).
Axes of the slice: x: 2, y: 2, z: 4, core: 2. Of those that a mesh axis runs over, the one named last changes fastest.
Arguments:
- activations: bfloat16 [2048, 28672], P('dp', 'tensor'), parts along dimension 0, may hold values from -6 to 6
- down_weight: bfloat16 [28672, 6144], P('tensor'), may hold values from -0.046875 to 0.046875
Outputs:
- projected: bfloat16 [2048, 6144], P(('dp', 'tensor')), parts along dimension 0
The draws below stay inside these ranges and needn't reach their ends.
There are 4 independent parts, one for each index of `dp`. The reference program is written for one: setup_inputs(seed, part) draws one part's arguments, and reference() takes and returns one part's arrays. A program takes and returns all parts, laid end to end along the dimension named above; an argument that names none is the same for every part. Nothing has to cross between parts.
All inputs are finite; a program needn't handle non-finite values.
Results may differ from the reference program's by a relative error of at most 0.015.
Values may be sent and summed in bfloat16 or wider, within the bound.
A program may use at most 128 MiB of HBM per device.

```python
import math
import jax
import jax.numpy as jnp
import numpy as np
from jax import lax

SYL = 1024
FF = 28672
DW = 6144
TOK = 512


def with_spikes(result, stream_key, source, target, blocks, factor):
    def block_of(position):
        return (jnp.arange(result.shape[position]) // (result.shape[position] // blocks)).reshape((-1,) + (1,) * (result.ndim - 1 - position))

    near = jax.random.permutation(stream_key, blocks)[block_of(target)]
    far = (block_of(target) + blocks // 2) % blocks
    return jnp.where((block_of(source) == near) | (block_of(source) == far), factor * result, result)


def level_of(stream_key, extent, cuts, smallest, top_value):
    loudness, own = 1.0, jax.random.fold_in(stream_key, 6)
    for position, parts in cuts:
        draws = jnp.exp(jax.random.uniform(jax.random.fold_in(own, position), (parts,), jnp.float32, smallest / len(cuts), top_value / len(cuts)))
        loudness = loudness * jnp.repeat(draws, extent[position] // parts).reshape([-1 if axis == position else 1 for axis in range(len(extent))])
    return loudness


def normal_values(own_key, dims, scale, limit, cuts=(), held_as=jnp.bfloat16):
    gain = level_of(own_key, dims, cuts, -0.22, 0.18) if cuts else 1.0
    values = jax.random.normal(own_key, dims, jnp.float32) * scale * gain
    return jnp.minimum(jnp.maximum(values, -limit), limit).astype(held_as)


def noise_with(own_key, extent, scale, reach, shards, heavy, dtype=jnp.bfloat16):
    result = scale * jax.random.normal(own_key, extent, jnp.float32)
    if shards:
        result = result * level_of(own_key, extent, shards, -0.22, 0.18)
    return jnp.clip(with_spikes(result, jax.random.fold_in(own_key, 3), *heavy), -reach, reach).astype(dtype)


def setup_inputs(seed: int = 0, part: int = 0) -> dict:
    arg_keys = jax.random.split(jax.random.key(seed), 3)
    own_keys = jax.random.split(jax.random.fold_in(arg_keys[2], part), 3)
    return {
        "activations": normal_values(own_keys[0], (TOK, FF), 1.0, 6.0, ((1, 8),)),
        "down_weight": noise_with(arg_keys[1], (FF, DW), FF ** -0.5, 0.046875, ((0, 8),), (0, 1, 8, 2.0)),
    }


def paley_matrix():
    modulus = 13
    residues = set((value * value % modulus for value in range(1, modulus)))
    jacobsthal = np.array([[0.0 if row_at == col_at else 1.0 if (col_at - row_at) % modulus in residues else -1.0 for col_at in range(modulus)] for row_at in range(modulus)])
    confer = np.zeros((14, 14))
    confer[0, 1:] = 1.0
    confer[1:, 0] = 1.0
    confer[1:, 1:] = jacobsthal
    return np.kron(confer, np.array([[1.0, 1.0], [1.0, -1.0]])) + np.kron(np.eye(14), np.array([[1.0, -1.0], [-1.0, -1.0]]))

def sylvester(order):
    matrix = np.ones((1, 1))
    while matrix.shape[0] < order:
        matrix = np.kron(matrix, np.array([[1.0, 1.0], [1.0, -1.0]]))
    return matrix

def quantize(rotated, largest):
    token_scale = jnp.maximum(largest, 1.0)
    levels = 7.0 * rotated / token_scale
    snapped = levels - jnp.sin(2.0 * math.pi * levels) / (2.0 * math.pi)
    return (snapped * token_scale / 7.0).astype(jnp.bfloat16)

def reference(activations, down_weight):
    count_rows = activations.shape[0]
    small_table = jnp.asarray(paley_matrix(), jnp.float32)
    power_table = jnp.asarray(sylvester(SYL), jnp.float32)
    values = activations.astype(jnp.float32).reshape(count_rows * SYL, 28)
    inner = jnp.dot(values, small_table, precision=lax.Precision.HIGHEST).reshape(count_rows, SYL, 28)
    outer = jnp.einsum('tji,jk->tki', inner, power_table, precision=lax.Precision.HIGHEST)
    rotated = outer.reshape(count_rows, FF) * (1.0 / math.sqrt(FF))
    largest = lax.optimization_barrier(jnp.max(jnp.abs(rotated), axis=1, keepdims=True))
    dequant = quantize(rotated, largest)
    return jnp.dot(dequant, down_weight, preferred_element_type=jnp.float32).astype(jnp.bfloat16)
```

```python
import functools
import math

import jax
import jax.numpy as jnp
import numpy as np
from jax import lax
from jax.experimental import pallas as pl
from jax.experimental.pallas import tpu as pltpu
from jax.sharding import PartitionSpec as P

INNER = 32
RESIDENT = 7
STREAM = 2
SECTIONS = 6
AHEAD = 2
BEHIND = 1
HOLD = 3


def paley_matrix():
    modulus = 13
    residues = set((value * value % modulus for value in range(1, modulus)))
    jacobsthal = np.array(
        [
            [
                (
                    0.0
                    if row_at == col_at
                    else 1.0 if (col_at - row_at) % modulus in residues else -1.0
                )
                for col_at in range(modulus)
            ]
            for row_at in range(modulus)
        ]
    )
    confer = np.zeros((14, 14))
    confer[0, 1:] = 1.0
    confer[1:, 0] = 1.0
    confer[1:, 1:] = jacobsthal
    return np.kron(confer, np.array([[1.0, 1.0], [1.0, -1.0]])) + np.kron(
        np.eye(14), np.array([[1.0, -1.0], [-1.0, -1.0]])
    )


def sylvester(order):
    matrix = np.ones((1, 1))
    while matrix.shape[0] < order:
        matrix = np.kron(matrix, np.array([[1.0, 1.0], [1.0, -1.0]]))
    return matrix


def sine_terms():
    series = np.polynomial.chebyshev.Chebyshev.interpolate(
        lambda square: np.sinc(2.0 * np.sqrt(np.maximum(square, 0.0))), 8, domain=[0.0, 0.25]
    )
    power = series.convert(kind=np.polynomial.Polynomial, domain=[-1, 1], window=[-1, 1])
    return [float(value) for value in power.coef]


def butterfly(values):
    step = 1
    while step < len(values):
        result = list(values)
        for at in range(len(values)):
            if not at & step:
                result[at] = values[at] + values[at + step]
                result[at + step] = values[at] - values[at + step]
        values, step = result, step * 2
    return values


def flipped(position, mask):
    result, bit = position, 1
    while bit <= mask:
        if mask & bit:
            result = result + (1 - 2 * ((position // bit) % 2)) * bit
        bit *= 2
    return result


def mirrored(position, groups):
    result, bit = 0, 1
    while bit < groups:
        result = result + ((position // bit) % 2) * (groups // 2 // bit)
        bit *= 2
    return result


def kernel(
    groups, chunks, tile, normal_scale, terms,
    act_ref, weight_ref, table_hbm, out_ref,
    table_ref, x_buf, rot, d_buf, flat, part, w_buf, *rest,
):
    stages = groups.bit_length() - 1
    recv_bufs = rest[:stages]
    (sent_sem, x_recv, q_recv, r_send, r_recv, last_recv, w_sem, t_sem) = rest[stages:]
    me = lax.axis_index("tensor")
    rows = x_buf.shape[2]
    width = x_buf.shape[3]
    inner = table_ref.shape[0]
    subs = width // inner
    features = weight_ref.shape[1]
    tiles = features // tile
    section_tiles = tiles // SECTIONS
    section_width = section_tiles * tile
    final = chunks - 1
    slots = part.shape[0]
    lags = [*range(1, stages - 1), stages, stages + 2]
    place = mirrored(me, groups)
    peers = [(mask, flipped(me, mask)) for mask in range(1, groups)]

    streamed = tiles - RESIDENT

    def weight_copy(at, slot):
        column = pl.multiple_of(at * tile, 128)
        return pltpu.make_async_copy(
            weight_ref.at[:, pl.ds(column, tile)], w_buf.at[slot], w_sem.at[slot]
        )

    def stream_copy(step):
        return weight_copy(RESIDENT + step % streamed, RESIDENT + step % STREAM)

    def own_rows(chunk):
        first = pl.multiple_of(me * (chunks * rows) + chunk * rows, rows)
        return pltpu.make_async_copy(
            act_ref.at[pl.ds(first, rows), :], x_buf.at[chunk, me], x_recv.at[chunk]
        )

    def x_copy(chunk, peer):
        first = pl.multiple_of(peer * (chunks * rows) + chunk * rows, rows)
        return pltpu.make_async_remote_copy(
            src_ref=act_ref.at[pl.ds(first, rows), :],
            dst_ref=x_buf.at[chunk, me],
            send_sem=sent_sem.at[chunk],
            recv_sem=x_recv.at[chunk],
            device_id={"tensor": peer},
            device_id_type=pl.DeviceIdType.MESH,
        )

    def q_copy(chunk, peer):
        return pltpu.make_async_remote_copy(
            src_ref=x_buf.at[chunk, peer],
            dst_ref=d_buf.at[chunk, place],
            send_sem=sent_sem.at[chunk],
            recv_sem=q_recv.at[chunk],
            device_id={"tensor": peer},
            device_id_type=pl.DeviceIdType.MESH,
        )

    def whole(ref, sem):
        return pltpu.make_async_copy(ref, ref, sem)

    def half_at(stage):
        start, span, kept = 0, groups, 0
        for at in range(stage + 1):
            span //= 2
            start = kept
            bit = (me // (1 << at)) % 2
            kept = start + bit * span
            sent = start + (1 - bit) * span
        return kept, sent, span

    def r_copy(chunk, stage, section=None, sem=None):
        kept, sent, span = half_at(stage)
        first, extent = 0, features
        if section is not None:
            first, extent = pl.multiple_of(section * section_width, 128), section_width
        column = pl.ds(first, extent)
        return pltpu.make_async_remote_copy(
            src_ref=part.at[chunk % slots, pl.ds(sent, span), :, column],
            dst_ref=recv_bufs[stage].at[chunk, :, :, column],
            send_sem=r_send.at[chunk],
            recv_sem=r_recv.at[chunk, stage] if sem is None else sem,
            device_id={"tensor": flipped(me, 1 << stage)},
            device_id_type=pl.DeviceIdType.MESH,
        )

    barrier = pltpu.get_barrier_semaphore()
    for mask, peer in peers:
        pl.semaphore_signal(
            barrier, inc=1, device_id={"tensor": peer}, device_id_type=pl.DeviceIdType.MESH
        )
    pl.semaphore_wait(barrier, groups - 1)

    def exchange(chunk):
        for mask, peer in peers:
            x_copy(chunk, peer).start()
        own_rows(chunk).start()

    for chunk in range(min(AHEAD, chunks)):
        exchange(chunk)
    table_copy = pltpu.make_async_copy(table_hbm, table_ref, t_sem)
    table_copy.start()
    table_copy.wait()
    for at in range(RESIDENT):
        weight_copy(at, at).start()
    for step in range(STREAM):
        stream_copy(step).start()

    def rotate(chunk):
        for sub in range(subs):
            block = x_buf[chunk, :, :, sub * inner:(sub + 1) * inner]
            rot[sub] = jnp.dot(
                block.reshape(groups * rows, inner), table_ref[...],
                preferred_element_type=jnp.float32,
            ).reshape(groups, rows, inner)

        def mix(at, tops):
            column = pl.ds(pl.multiple_of(at * 128, 128), 128)
            result = []
            for index in range(rows // 8):
                line = pl.ds(index * 8, 8)
                values = butterfly(
                    [rot[sub, group, line, column] for group in range(groups) for sub in range(subs)]
                )
                top = tops[index]
                for block_at, value in enumerate(values):
                    rot[block_at % subs, block_at // subs, line, column] = value
                    top = jnp.maximum(top, jnp.abs(value))
                result.append(top)
            return tuple(result)

        tops = lax.fori_loop(
            0, inner // 128, mix,
            tuple(jnp.zeros((8, 128), jnp.float32) for _ in range(rows // 8)),
        )
        largest = jnp.concatenate([jnp.max(top, axis=1, keepdims=True) for top in tops], axis=0)
        token_scale = jnp.maximum(largest * normal_scale, 1.0)
        into = 7.0 * normal_scale / token_scale
        back = token_scale / 7.0

        @pl.loop(0, groups)
        def _(group):
            for sub in range(subs):
                levels = rot[sub, group] * into
                offset = levels - jnp.floor(levels + 0.5)
                square = offset * offset
                series = jnp.full_like(square, terms[-1])
                for term in terms[-2::-1]:
                    series = series * square + term
                x_buf[chunk, group, :, sub * inner:(sub + 1) * inner] = (
                    (levels - offset * series) * back
                ).astype(jnp.bfloat16)

    def finish_tokens(chunk):
        whole(x_buf.at[chunk], x_recv.at[chunk]).wait()
        rotate(chunk)
        d_buf[chunk, place] = x_buf[chunk, me]
        for mask, peer in peers:
            q_copy(chunk, peer).start()

        @pl.when(chunk + AHEAD < chunks)
        def _():
            exchange(chunk + AHEAD)

    def add_up(chunk, stage, first, extent):
        kept, sent, span = half_at(stage)
        pieces = extent // section_width

        @pl.loop(0, span * pieces)
        def _(at):
            block = at // pieces
            column = pl.ds(pl.multiple_of(first + (at % pieces) * section_width, 128), section_width)
            total = (
                part[chunk % slots, kept + block, :, column].astype(jnp.float32)
                + recv_bufs[stage][chunk, block, :, column].astype(jnp.float32)
            ).astype(jnp.bfloat16)
            if stage == stages - 1:
                out_ref[pl.ds(pl.multiple_of(chunk * rows, rows), rows), column] = total
            else:
                part[chunk % slots, kept + block, :, column] = total

    def reduce_chunk(chunk, stage):
        whole(recv_bufs[stage].at[chunk], r_recv.at[chunk, stage]).wait()
        add_up(chunk, stage, 0, features)
        if stage < stages - 1:
            r_copy(chunk, stage + 1).start()

    def reduce_last(stage, section):
        r_copy(final, stage, section, last_recv.at[stage, section]).wait_recv()
        add_up(final, stage, section * section_width, section_width)
        if stage < stages - 1:
            r_copy(final, stage + 1, section, last_recv.at[stage + 1, section]).start()

    def product(chunk, at, slot):
        part[chunk % slots, :, :, pl.ds(pl.multiple_of(at * tile, 128), tile)] = (
            jnp.dot(
                flat[...],
                w_buf[slot],
                preferred_element_type=jnp.float32,
            )
            .astype(jnp.bfloat16)
            .reshape(groups, rows, tile)
        )

    def multiply(chunk, section):
        @pl.loop(section * section_tiles, (section + 1) * section_tiles)
        def _(at):
            step = chunk * streamed + at - RESIDENT

            @pl.when((chunk == 0) & (at < RESIDENT))
            def _():
                weight_copy(at, at).wait()

            if streamed:
                @pl.when(at >= RESIDENT)
                def _():
                    stream_copy(step).wait()

                resident = at // RESIDENT
                product(chunk, at, (1 - resident) * at + resident * (RESIDENT + step % STREAM))

                @pl.when((at >= RESIDENT) & (step + STREAM < chunks * streamed))
                def _():
                    stream_copy(step + STREAM).start()
            else:
                product(chunk, at, at)

    def sends_done(chunk):
        whole(part.at[chunk % slots, pl.ds(0, groups - 1)], r_send.at[chunk]).wait()

    def gather(chunk):
        others = pl.ds(0, groups - 1)
        whole(d_buf.at[chunk, others], q_recv.at[chunk]).wait()
        flat[...] = d_buf[chunk].reshape(groups * rows, width)

    @pl.loop(0, final + BEHIND)
    def _(turn):
        @pl.when(turn < chunks)
        def _():
            finish_tokens(turn)

        @pl.when(turn >= BEHIND)
        def _():
            chunk = turn - BEHIND
            gather(chunk)

            @pl.when(chunk >= slots)
            def _():
                sends_done(chunk - slots)

            for stage in range(stages):
                @pl.when(chunk >= lags[stage])
                def _():
                    reduce_chunk(chunk - lags[stage], stage)

            @pl.loop(0, SECTIONS)
            def _(section):
                multiply(chunk, section)
                r_copy(chunk, 0, section).start()

    def reduce_back(most, least, stage):
        for back in range(min(most, final), least - 1, -1):
            reduce_chunk(final - back, stage)

    gather(final)
    if final >= slots:
        sends_done(final - slots)
        reduce_chunk(final - slots, stages - 1)
    for stage in range(stages - 2, 0, -1):
        reduce_back(lags[stage], stage + 1, stage)

    @pl.loop(0, SECTIONS)
    def _(section):
        multiply(final, section)
        r_copy(final, 0, section, last_recv.at[0, section]).start()

        @pl.when(section == HOLD - 1)
        def _():
            reduce_back(1, 1, 0)

        @pl.when(section >= HOLD)
        def _():
            reduce_last(0, section - HOLD)

    reduce_last(0, SECTIONS - HOLD)
    for stage in range(1, stages - 1):
        reduce_back(stage, 1, stage)
        for section in range(SECTIONS):
            if stage == 1 and section + 1 < HOLD:
                reduce_last(0, SECTIONS - HOLD + 1 + section)
            reduce_last(stage, section)
    reduce_back(slots - 1, 1, stages - 1)

    @pl.loop(0, SECTIONS)
    def _(section):
        reduce_last(stages - 1, section)

    @pl.loop(0, chunks)
    def _(chunk):
        whole(x_buf.at[pl.ds(0, 2), pl.ds(0, groups - 1)], sent_sem.at[chunk]).wait()

    @pl.loop(chunks - slots, chunks)
    def _(chunk):
        sends_done(chunk)


def shards(activations, down_weight):
    count_rows, width = activations.shape
    features = down_weight.shape[1]
    groups = lax.axis_size("tensor")
    stages = groups.bit_length() - 1
    own = count_rows // groups
    rows = 8
    chunks = own // rows
    tile = 512
    table = jnp.asarray(np.kron(sylvester(INNER), paley_matrix()), jnp.bfloat16)
    inner = table.shape[0]
    bf16, dma = jnp.bfloat16, pltpu.SemaphoreType.DMA
    body = functools.partial(
        kernel, groups, chunks, tile, 1.0 / math.sqrt(width * groups), sine_terms()
    )
    return pl.pallas_call(
        body,
        out_shape=jax.ShapeDtypeStruct((own, features), bf16),
        in_specs=[
            pl.BlockSpec(memory_space=pltpu.HBM),
            pl.BlockSpec(memory_space=pltpu.HBM),
            pl.BlockSpec(memory_space=pltpu.HBM),
        ],
        out_specs=pl.BlockSpec(memory_space=pltpu.VMEM),
        scratch_shapes=[
            pltpu.VMEM((inner, inner), bf16),
            pltpu.VMEM((chunks, groups, rows, width), bf16),
            pltpu.VMEM((width // inner, groups, rows, inner), jnp.float32),
            pltpu.VMEM((chunks, groups, rows, width), bf16),
            pltpu.VMEM((groups * rows, width), bf16),
            pltpu.VMEM((min(stages + 2, chunks), groups, rows, features), bf16),
            pltpu.VMEM((RESIDENT + STREAM, width, tile), bf16),
        ]
        + [
            pltpu.VMEM((chunks, groups >> (stage + 1), rows, features), bf16)
            for stage in range(stages)
        ]
        + [
            dma((chunks,)),
            dma((chunks,)),
            dma((chunks,)),
            dma((chunks,)),
            dma((chunks, stages)),
            dma((stages, SECTIONS)),
            dma((RESIDENT + STREAM,)),
            dma,
        ],
        compiler_params=pltpu.CompilerParams(
            collective_id=0, has_side_effects=True, vmem_limit_bytes=53 * 1024 * 1024
        ),
        name="rotate_quantize_project",
    )(activations, down_weight, table)


def solution(mesh):
    placed = (P("dp", "tensor"), P("tensor", None))
    return jax.shard_map(
        shards, mesh=mesh, in_specs=placed, out_specs=P(("dp", "tensor"), None), check_vma=False
    )
```

```python
import functools
import math

import jax
import jax.numpy as jnp
import numpy as np
from jax import lax
from jax.experimental import pallas as pl
from jax.experimental.pallas import tpu as pltpu
from jax.sharding import PartitionSpec as P

INNER = 32
RESIDENT = 7
STREAM = 2
SECTIONS = 6
AHEAD = 2
BEHIND = 1
HOLD = 3


def paley_matrix():
    modulus = 13
    residues = set((value * value % modulus for value in range(1, modulus)))
    jacobsthal = np.array(
        [
            [
                (
                    0.0
                    if row_at == col_at
                    else 1.0 if (col_at - row_at) % modulus in residues else -1.0
                )
                for col_at in range(modulus)
            ]
            for row_at in range(modulus)
        ]
    )
    confer = np.zeros((14, 14))
    confer[0, 1:] = 1.0
    confer[1:, 0] = 1.0
    confer[1:, 1:] = jacobsthal
    return np.kron(confer, np.array([[1.0, 1.0], [1.0, -1.0]])) + np.kron(
        np.eye(14), np.array([[1.0, -1.0], [-1.0, -1.0]])
    )


def sylvester(order):
    matrix = np.ones((1, 1))
    while matrix.shape[0] < order:
        matrix = np.kron(matrix, np.array([[1.0, 1.0], [1.0, -1.0]]))
    return matrix


def sine_terms():
    series = np.polynomial.chebyshev.Chebyshev.interpolate(
        lambda square: np.sinc(2.0 * np.sqrt(np.maximum(square, 0.0))), 8, domain=[0.0, 0.25]
    )
    power = series.convert(kind=np.polynomial.Polynomial, domain=[-1, 1], window=[-1, 1])
    return [float(value) for value in power.coef]


def butterfly(values):
    step = 1
    while step < len(values):
        result = list(values)
        for at in range(len(values)):
            if not at & step:
                result[at] = values[at] + values[at + step]
                result[at + step] = values[at] - values[at + step]
        values, step = result, step * 2
    return values


def flipped(position, mask):
    result, bit = position, 1
    while bit <= mask:
        if mask & bit:
            result = result + (1 - 2 * ((position // bit) % 2)) * bit
        bit *= 2
    return result


def mirrored(position, groups):
    result, bit = 0, 1
    while bit < groups:
        result = result + ((position // bit) % 2) * (groups // 2 // bit)
        bit *= 2
    return result


def kernel(
    groups, chunks, tile, normal_scale, terms,
    act_ref, weight_ref, table_hbm, out_ref,
    table_ref, x_buf, rot, d_buf, flat, part, w_buf, *rest,
):
    stages = groups.bit_length() - 1
    recv_bufs = rest[:stages]
    (sent_sem, x_recv, q_recv, r_send, r_recv, last_recv, w_sem, t_sem) = rest[stages:]
    me = lax.axis_index("tensor")
    rows = x_buf.shape[2]
    width = x_buf.shape[3]
    inner = table_ref.shape[0]
    subs = width // inner
    features = weight_ref.shape[1]
    tiles = features // tile
    section_tiles = tiles // SECTIONS
    section_width = section_tiles * tile
    final = chunks - 1
    slots = part.shape[0]
    lags = [*range(1, stages - 1), stages, stages + 2]
    place = mirrored(me, groups)
    peers = [(mask, flipped(me, mask)) for mask in range(1, groups)]

    streamed = tiles - RESIDENT

    def weight_copy(at, slot):
        column = pl.multiple_of(at * tile, 128)
        return pltpu.make_async_copy(
            weight_ref.at[:, pl.ds(column, tile)], w_buf.at[slot], w_sem.at[slot]
        )

    def stream_copy(step):
        return weight_copy(2 * (step % streamed) + 1, RESIDENT + step % STREAM)

    def own_rows(chunk):
        first = pl.multiple_of(me * (chunks * rows) + chunk * rows, rows)
        return pltpu.make_async_copy(
            act_ref.at[pl.ds(first, rows), :], x_buf.at[chunk, me], x_recv.at[chunk]
        )

    def x_copy(chunk, peer):
        first = pl.multiple_of(peer * (chunks * rows) + chunk * rows, rows)
        return pltpu.make_async_remote_copy(
            src_ref=act_ref.at[pl.ds(first, rows), :],
            dst_ref=x_buf.at[chunk, me],
            send_sem=sent_sem.at[chunk],
            recv_sem=x_recv.at[chunk],
            device_id={"tensor": peer},
            device_id_type=pl.DeviceIdType.MESH,
        )

    def q_copy(chunk, peer):
        return pltpu.make_async_remote_copy(
            src_ref=x_buf.at[chunk, peer],
            dst_ref=d_buf.at[chunk, place],
            send_sem=sent_sem.at[chunk],
            recv_sem=q_recv.at[chunk],
            device_id={"tensor": peer},
            device_id_type=pl.DeviceIdType.MESH,
        )

    def whole(ref, sem):
        return pltpu.make_async_copy(ref, ref, sem)

    def half_at(stage):
        start, span, kept = 0, groups, 0
        for at in range(stage + 1):
            span //= 2
            start = kept
            bit = (me // (1 << at)) % 2
            kept = start + bit * span
            sent = start + (1 - bit) * span
        return kept, sent, span

    def r_copy(chunk, stage, section=None, sem=None):
        kept, sent, span = half_at(stage)
        first, extent = 0, features
        if section is not None:
            first, extent = pl.multiple_of(section * section_width, 128), section_width
        column = pl.ds(first, extent)
        return pltpu.make_async_remote_copy(
            src_ref=part.at[chunk % slots, pl.ds(sent, span), :, column],
            dst_ref=recv_bufs[stage].at[chunk, :, :, column],
            send_sem=r_send.at[chunk],
            recv_sem=r_recv.at[chunk, stage] if sem is None else sem,
            device_id={"tensor": flipped(me, 1 << stage)},
            device_id_type=pl.DeviceIdType.MESH,
        )

    barrier = pltpu.get_barrier_semaphore()
    for mask, peer in peers:
        pl.semaphore_signal(
            barrier, inc=1, device_id={"tensor": peer}, device_id_type=pl.DeviceIdType.MESH
        )
    pl.semaphore_wait(barrier, groups - 1)

    def exchange(chunk):
        for mask, peer in peers:
            x_copy(chunk, peer).start()
        own_rows(chunk).start()

    for chunk in range(min(AHEAD, chunks)):
        exchange(chunk)
    table_copy = pltpu.make_async_copy(table_hbm, table_ref, t_sem)
    table_copy.start()
    table_copy.wait()
    for at in range(tiles):
        if at % 2 == 0 or at > 2 * streamed:
            weight_copy(at, at - min(at // 2, streamed)).start()
        elif at // 2 < STREAM:
            stream_copy(at // 2).start()

    def rotate(chunk):
        for sub in range(subs):
            block = x_buf[chunk, :, :, sub * inner:(sub + 1) * inner]
            rot[sub] = jnp.dot(
                block.reshape(groups * rows, inner), table_ref[...],
                preferred_element_type=jnp.float32,
            ).reshape(groups, rows, inner)

        def mix(at, tops):
            column = pl.ds(pl.multiple_of(at * 128, 128), 128)
            result = []
            for index in range(rows // 8):
                line = pl.ds(index * 8, 8)
                values = butterfly(
                    [rot[sub, group, line, column] for group in range(groups) for sub in range(subs)]
                )
                top = tops[index]
                for block_at, value in enumerate(values):
                    rot[block_at % subs, block_at // subs, line, column] = value
                    top = jnp.maximum(top, jnp.abs(value))
                result.append(top)
            return tuple(result)

        tops = lax.fori_loop(
            0, inner // 128, mix,
            tuple(jnp.zeros((8, 128), jnp.float32) for _ in range(rows // 8)),
        )
        largest = jnp.concatenate([jnp.max(top, axis=1, keepdims=True) for top in tops], axis=0)
        token_scale = jnp.maximum(largest * normal_scale, 1.0)
        into = 7.0 * normal_scale / token_scale
        back = token_scale / 7.0

        @pl.loop(0, groups)
        def _(group):
            for sub in range(subs):
                levels = rot[sub, group] * into
                offset = levels - jnp.floor(levels + 0.5)
                square = offset * offset
                series = jnp.full_like(square, terms[-1])
                for term in terms[-2::-1]:
                    series = series * square + term
                x_buf[chunk, group, :, sub * inner:(sub + 1) * inner] = (
                    (levels - offset * series) * back
                ).astype(jnp.bfloat16)

    def finish_tokens(chunk):
        whole(x_buf.at[chunk], x_recv.at[chunk]).wait()
        rotate(chunk)
        d_buf[chunk, place] = x_buf[chunk, me]
        for mask, peer in peers:
            q_copy(chunk, peer).start()

        @pl.when(chunk + AHEAD < chunks)
        def _():
            exchange(chunk + AHEAD)

    def add_up(chunk, stage, first, extent):
        kept, sent, span = half_at(stage)
        pieces = extent // section_width

        @pl.loop(0, span * pieces)
        def _(at):
            block = at // pieces
            column = pl.ds(pl.multiple_of(first + (at % pieces) * section_width, 128), section_width)
            total = (
                part[chunk % slots, kept + block, :, column].astype(jnp.float32)
                + recv_bufs[stage][chunk, block, :, column].astype(jnp.float32)
            ).astype(jnp.bfloat16)
            if stage == stages - 1:
                out_ref[pl.ds(pl.multiple_of(chunk * rows, rows), rows), column] = total
            else:
                part[chunk % slots, kept + block, :, column] = total

    def reduce_chunk(chunk, stage):
        whole(recv_bufs[stage].at[chunk], r_recv.at[chunk, stage]).wait()
        add_up(chunk, stage, 0, features)
        if stage < stages - 1:
            r_copy(chunk, stage + 1).start()

    def reduce_last(stage, section):
        r_copy(final, stage, section, last_recv.at[stage, section]).wait_recv()
        add_up(final, stage, section * section_width, section_width)
        if stage < stages - 1:
            r_copy(final, stage + 1, section, last_recv.at[stage + 1, section]).start()

    def product(chunk, at, slot):
        part[chunk % slots, :, :, pl.ds(pl.multiple_of(at * tile, 128), tile)] = (
            jnp.dot(
                flat[...],
                w_buf[slot],
                preferred_element_type=jnp.float32,
            )
            .astype(jnp.bfloat16)
            .reshape(groups, rows, tile)
        )

    def multiply(chunk, section):
        @pl.loop(section * section_tiles, (section + 1) * section_tiles)
        def _(at):
            pair, odd = at // 2, at % 2
            paired = 1 - at // (2 * streamed)
            passing = odd * paired
            step = chunk * streamed + pair
            kept = paired * pair + (1 - paired) * (at - streamed)

            @pl.when((chunk == 0) & (passing == 0))
            def _():
                weight_copy(at, kept).wait()

            @pl.when(passing == 1)
            def _():
                stream_copy(step).wait()

            product(chunk, at, (1 - passing) * kept + passing * (RESIDENT + step % STREAM))

            @pl.when((passing == 1) & (step + STREAM < chunks * streamed))
            def _():
                stream_copy(step + STREAM).start()

    def sends_done(chunk):
        whole(part.at[chunk % slots, pl.ds(0, groups - 1)], r_send.at[chunk]).wait()

    def gather(chunk):
        others = pl.ds(0, groups - 1)
        whole(d_buf.at[chunk, others], q_recv.at[chunk]).wait()
        flat[...] = d_buf[chunk].reshape(groups * rows, width)

    @pl.loop(0, final + BEHIND)
    def _(turn):
        @pl.when(turn < chunks)
        def _():
            finish_tokens(turn)

        @pl.when(turn >= BEHIND)
        def _():
            chunk = turn - BEHIND
            gather(chunk)

            @pl.when(chunk >= slots)
            def _():
                sends_done(chunk - slots)

            for stage in range(stages):
                @pl.when(chunk >= lags[stage])
                def _():
                    reduce_chunk(chunk - lags[stage], stage)

            @pl.loop(0, SECTIONS)
            def _(section):
                multiply(chunk, section)
                r_copy(chunk, 0, section).start()

    def reduce_back(most, least, stage):
        for back in range(min(most, final), least - 1, -1):
            reduce_chunk(final - back, stage)

    gather(final)
    if final >= slots:
        sends_done(final - slots)
        reduce_chunk(final - slots, stages - 1)
    for stage in range(stages - 2, 0, -1):
        reduce_back(lags[stage], stage + 1, stage)

    @pl.loop(0, SECTIONS)
    def _(section):
        multiply(final, section)
        r_copy(final, 0, section, last_recv.at[0, section]).start()

        @pl.when(section == 1)
        def _():
            reduce_back(1, 1, 0)

        @pl.when(section >= HOLD)
        def _():
            reduce_last(0, section - HOLD)

    reduce_last(0, SECTIONS - HOLD)
    for stage in range(1, stages - 1):
        reduce_back(stage, 1, stage)
        for section in range(SECTIONS):
            if stage == 1 and section + 1 < HOLD:
                reduce_last(0, SECTIONS - HOLD + 1 + section)
            reduce_last(stage, section)
    reduce_back(slots - 1, 1, stages - 1)

    @pl.loop(0, SECTIONS)
    def _(section):
        reduce_last(stages - 1, section)

    @pl.loop(0, chunks)
    def _(chunk):
        whole(x_buf.at[pl.ds(0, 2), pl.ds(0, groups - 1)], sent_sem.at[chunk]).wait()

    @pl.loop(chunks - slots, chunks)
    def _(chunk):
        sends_done(chunk)


def shards(activations, down_weight):
    count_rows, width = activations.shape
    features = down_weight.shape[1]
    groups = lax.axis_size("tensor")
    stages = groups.bit_length() - 1
    own = count_rows // groups
    rows = 8
    chunks = own // rows
    tile = 512
    table = jnp.asarray(np.kron(sylvester(INNER), paley_matrix()), jnp.bfloat16)
    inner = table.shape[0]
    bf16, dma = jnp.bfloat16, pltpu.SemaphoreType.DMA
    body = functools.partial(
        kernel, groups, chunks, tile, 1.0 / math.sqrt(width * groups), sine_terms()
    )
    return pl.pallas_call(
        body,
        out_shape=jax.ShapeDtypeStruct((own, features), bf16),
        in_specs=[
            pl.BlockSpec(memory_space=pltpu.HBM),
            pl.BlockSpec(memory_space=pltpu.HBM),
            pl.BlockSpec(memory_space=pltpu.HBM),
        ],
        out_specs=pl.BlockSpec(memory_space=pltpu.VMEM),
        scratch_shapes=[
            pltpu.VMEM((inner, inner), bf16),
            pltpu.VMEM((chunks, groups, rows, width), bf16),
            pltpu.VMEM((width // inner, groups, rows, inner), jnp.float32),
            pltpu.VMEM((chunks, groups, rows, width), bf16),
            pltpu.VMEM((groups * rows, width), bf16),
            pltpu.VMEM((min(stages + 2, chunks), groups, rows, features), bf16),
            pltpu.VMEM((RESIDENT + STREAM, width, tile), bf16),
        ]
        + [
            pltpu.VMEM((chunks, groups >> (stage + 1), rows, features), bf16)
            for stage in range(stages)
        ]
        + [
            dma((chunks,)),
            dma((chunks,)),
            dma((chunks,)),
            dma((chunks,)),
            dma((chunks, stages)),
            dma((stages, SECTIONS)),
            dma((RESIDENT + STREAM,)),
            dma,
        ],
        compiler_params=pltpu.CompilerParams(
            collective_id=0, has_side_effects=True, vmem_limit_bytes=53 * 1024 * 1024
        ),
        name="rotate_quantize_project",
    )(activations, down_weight, table)


def solution(mesh):
    placed = (P("dp", "tensor"), P("tensor", None))
    return jax.shard_map(
        shards, mesh=mesh, in_specs=placed, out_specs=P(("dp", "tensor"), None), check_vma=False
    )
```
